128 devices in a mesh: member: 64 (over z, y, x), domain: 2 (over core).
Axes of the slice: x: 4, y: 4, z: 4, core: 2. Of those that a mesh axis runs over, the one named last changes fastest.
Arguments:
- state: bfloat16 [512, 131072], P('member', 'domain'), may hold values from -6 to 6
- predicted: bfloat16 [512, 262144], P('member', 'domain'), may hold values from -6 to 6
- perturbed: bfloat16 [512, 262144], P('member', 'domain'), may hold values from -6 to 6
- obs_weight: float32 [262144], P('domain'), may hold values from 0.3 to 3
- obs_position: int32 [262144], P('domain'), may hold values from 0 to 255
- row_count: int32 [2, 128], P(None, 'member'), may hold values from 256 to 2048
- row_index: int32 [2, 128, 2048], P('domain', 'member'), may hold values from 0 to 2047, as said below
Outputs:
- updated: bfloat16 [512, 131072], P('member', 'domain')
The draws below stay inside these ranges and needn't reach their ends.
Inputs may be any that keep to these rules, and one draw needn't show every extreme that they name: `row_index`: for each block, 2048 distinct rows of its pool; only the first row_count of them are used.
All inputs are finite; a program needn't handle non-finite values.
Results may differ from the reference program's by a relative error of at most 0.0054.
Values may be sent and summed in bfloat16 or wider, within the bound.
No kernel may reach another device: no remote copies, remote signals or barrier semaphores. Data moves between devices by JAX's collectives and lax.ppermute only.
A program may use at most 128 MiB of HBM per device.

```python
import math
import jax
import jax.numpy as jnp
from jax import lax

MEMBERS = 512
ROWCAP = 2048
ROWMIN = 256
POOL = 2048
BPD = 2
NS_STEPS = 5
SPAN = 2
TILES = 2
TILE_BLOCKS = 128
NBLOCKS = 256
CELLS = 131072
OBS = 262144


def draw_obs_position(key, part):
    base_block = jnp.arange(OBS, dtype=jnp.int32) // POOL * BPD
    shifted = jax.random.randint(key, (OBS,), -2 * SPAN, BPD + 2 * SPAN, dtype=jnp.int32)
    return jnp.clip(base_block + shifted, 0, NBLOCKS - 1).astype(jnp.int32)


def draw_row_count(key, part):
    levels = jax.random.randint(key, (TILES, TILE_BLOCKS), 0, 1024, dtype=jnp.int32)
    counts = ROWMIN + levels * levels * (ROWCAP - ROWMIN) // (1023 * 1023)
    counts = counts.at[0, 0].set(ROWCAP)
    counts = counts.at[0, 1].set(ROWMIN)
    return counts.astype(jnp.int32)


def draw_row_index(key, part):
    keys = jax.random.split(key, TILES * TILE_BLOCKS)

    def one_list(single_key):
        return jax.random.permutation(single_key, POOL)[:ROWCAP]
    lists = jax.vmap(one_list)(keys)
    return lists.reshape(TILES, TILE_BLOCKS, ROWCAP).astype(jnp.int32)


def steps_of(own_key, extent, cuts, least, largest):
    factor_of, own = 1.0, jax.random.fold_in(own_key, 6)
    for dim, shards_of in cuts:
        draws = jnp.exp(jax.random.uniform(jax.random.fold_in(own, dim), (shards_of,), jnp.float32, least / len(cuts), largest / len(cuts)))
        factor_of = factor_of * jnp.repeat(draws, extent[dim] // shards_of).reshape([-1 if axis == dim else 1 for axis in range(len(extent))])
    return factor_of


def noise(own_key, extent, scale, most, cuts=(), kind=jnp.bfloat16):
    values = jax.random.normal(own_key, extent, jnp.float32) * scale
    if len(cuts) > 0:
        values = steps_of(own_key, extent, cuts, -0.22, 0.18) * values
    return jnp.clip(values, min=-most, max=most).astype(kind)


def setup_inputs(seed: int = 0) -> dict:
    key_list = jax.random.split(jax.random.key(seed), 8)
    state = noise(key_list[0], (MEMBERS, CELLS), 1.0, 6.0, ((0, 64), (1, 2)))
    predicted = noise(key_list[1], (MEMBERS, OBS), 1.0, 6.0, ((0, 64), (1, 2)))
    perturbed = noise(key_list[2], (MEMBERS, OBS), 1.0, 6.0, ((0, 64), (1, 2)))
    obs_weight = jnp.clip(jnp.exp(math.log(3.0) - 2.3025851 * jax.random.uniform(key_list[3], (OBS,), jnp.float32) ** steps_of(key_list[3], (OBS,), ((0, 2),), -0.2, 0.2)), 0.3, 3.0)
    obs_position = draw_obs_position(jax.random.fold_in(key_list[7], 71), 0)
    row_count = draw_row_count(jax.random.fold_in(key_list[7], 71), 0)
    row_index = draw_row_index(jax.random.fold_in(key_list[7], 71), 0)
    return dict(state=state, predicted=predicted, perturbed=perturbed, obs_weight=obs_weight, obs_position=obs_position, row_count=row_count, row_index=row_index)


def scaled_rows(obs_pools, index_list, row_total, position, row_start, length):
    pred_pool, pert_pool, mean_pred, weight_pool, place_pool = obs_pools
    picked = lax.dynamic_slice_in_dim(index_list, row_start, length)
    pred_rows = jnp.take(pred_pool, picked, axis=0).astype(jnp.float32)
    pert_rows = jnp.take(pert_pool, picked, axis=0).astype(jnp.float32)
    offset = (jnp.take(place_pool, picked) - position).astype(jnp.float32) / SPAN
    taper_factor = 1.0 / (1.0 + offset * offset)
    live_rows = row_start + jnp.arange(length, dtype=jnp.int32) < row_total
    factor = jnp.where(live_rows, jnp.take(weight_pool, picked) * taper_factor, 0.0)
    members = pred_pool.shape[1]
    scaled = (factor[:, None] * (pred_rows - jnp.take(mean_pred, picked)[:, None]) / jnp.sqrt(members - 1.0)).astype(jnp.bfloat16)
    innovation = (factor[:, None] * (pert_rows - pred_rows)).astype(jnp.bfloat16)
    return (scaled, innovation)

def newton_inverse(gram_sum):
    members = gram_sum.shape[0]
    identity = jnp.eye(members, dtype=jnp.float32)
    system = identity + gram_sum
    spread = jnp.sqrt(jnp.sum(gram_sum * gram_sum))
    estimate = 2.0 / (2.0 + spread) * identity
    for iteration in range(NS_STEPS):
        product = jnp.dot(system, estimate, precision=lax.Precision.HIGHEST)
        estimate = jnp.dot(estimate, 2.0 * identity - product, precision=lax.Precision.HIGHEST)
    return estimate

def update_block(cell_block, gram_sum, cross_sum):
    members = gram_sum.shape[0]
    inverse = newton_inverse(gram_sum)
    weights = (jnp.dot(inverse, cross_sum, precision=lax.Precision.HIGHEST) / math.sqrt(members - 1.0)).astype(jnp.bfloat16)
    values = cell_block.astype(jnp.float32)
    centred = (values - lax.optimization_barrier(jnp.mean(values, axis=1, keepdims=True))).astype(jnp.bfloat16)
    change = jnp.dot(centred.astype(jnp.float32), weights.astype(jnp.float32), precision=lax.Precision.HIGHEST)
    return (values + change).astype(jnp.bfloat16)

def reference(state, predicted, perturbed, obs_weight, obs_position, row_count, row_index):
    cell_major = state.T
    pred_rows_all = predicted.T
    pert_rows_all = perturbed.T
    members = cell_major.shape[1]
    block_total = row_count.shape[0] * row_count.shape[1]
    counts = row_count.reshape(block_total)
    lists = row_index.reshape(block_total, row_index.shape[2])
    cell_blocks = cell_major.reshape(block_total, cell_major.shape[0] // block_total, members)
    mean_pred = lax.optimization_barrier(jnp.mean(pred_rows_all, axis=1, dtype=jnp.float32))
    obs_pools = (pred_rows_all, pert_rows_all, mean_pred, obs_weight, obs_position)

    def one_block(inputs):
        cell_block, index_list, row_total, number = inputs
        offset_rows = (number // BPD * POOL).astype(jnp.int32)
        scaled, innovation = scaled_rows(obs_pools, index_list + offset_rows, row_total, number, 0, index_list.shape[0])
        scaled_wide = scaled.astype(jnp.float32)
        innov_wide = innovation.astype(jnp.float32)
        gram_sum = jnp.dot(scaled_wide.T, scaled_wide, precision=lax.Precision.HIGHEST)
        cross_sum = jnp.dot(scaled_wide.T, innov_wide, precision=lax.Precision.HIGHEST)
        return update_block(cell_block, gram_sum, cross_sum)
    numbers = jnp.arange(block_total, dtype=jnp.int32)
    renewed = lax.map(one_block, (cell_blocks, lists, counts, numbers))
    return renewed.reshape(cell_major.shape).T
```

```python
import math

import jax
import jax.numpy as jnp
from jax import lax
from jax.experimental import pallas as pl
from jax.experimental.pallas import tpu as pltpu
from jax.sharding import PartitionSpec as P

NS_STEPS = 5
SPAN = 2
LANES = 128

f32 = jnp.float32
bf16 = jnp.bfloat16


def contract_lanes(left, right):
    return lax.dot_general(left, right, (((1,), (1,)), ((), ())), preferred_element_type=f32)


def dot(left, right):
    return jnp.dot(left, right, preferred_element_type=f32)


def split(value):
    high = value.astype(bf16)
    return high, (value - high.astype(f32)).astype(bf16)


def dot3(left, right):
    left_high, left_low = left
    right_high, right_low = right
    return dot(left_high, right_high) + (dot(left_high, right_low) + dot(left_low, right_high))


def factor_kernel(scalars, index, weight, place, factor_out):
    blocks, rows = index.shape
    tiles = rows // LANES
    for block in range(blocks):
        listed = index[block : block + 1, :]
        live = lax.broadcasted_iota(jnp.int32, (1, rows), 1) < scalars[1 + block]
        high = jnp.where(live, listed // LANES, -1)
        low = listed % LANES
        high_hot = (lax.broadcasted_iota(jnp.int32, (tiles, rows), 0) == high).astype(f32).astype(bf16)
        low_hot = (lax.broadcasted_iota(jnp.int32, (LANES, rows), 0) == low).astype(f32).astype(bf16)
        chosen = contract_lanes(high_hot, low_hot)
        chosen = jnp.concatenate([chosen[t : t + 1, :] for t in range(tiles)], axis=1)
        offset = (place[...] - (scalars[0] + block)).astype(f32) / SPAN
        taper = 1.0 / (1.0 + offset * offset)
        factor_out[block : block + 1, :] = jnp.where(chosen > 0.5, weight[...] * taper, 0.0)


def inverse_kernel(pred, factor, scaled_out, inverse_out):
    members = pred.shape[0]
    blocks = factor.shape[0]
    values = pred[...].astype(f32)
    deviation = values - jnp.mean(values, axis=0, keepdims=True)
    eye = (
        lax.broadcasted_iota(jnp.int32, (members, members), 0)
        == lax.broadcasted_iota(jnp.int32, (members, members), 1)
    ).astype(f32)
    for block in range(blocks):
        scaled = (factor[block : block + 1, :] * deviation * (1.0 / math.sqrt(members - 1.0))).astype(bf16)
        scaled_out[block] = scaled
        gram = contract_lanes(scaled, scaled)
        start = 2.0 / (2.0 + jnp.sqrt(jnp.sum(gram * gram)))
        residual = eye - start * (eye + gram)
        estimate = eye + residual
        residual_parts = split(residual)
        for step in range(1, NS_STEPS):
            residual = dot3(residual_parts, residual_parts)
            residual_parts = split(residual)
            estimate = estimate + dot3(split(estimate), residual_parts)
        inverse_out[block] = start * estimate


def weights_kernel(pred, pert, factor, scaled, inverse, weights_out):
    members = pred.shape[0]
    change = pert[...].astype(f32) - pred[...].astype(f32)
    for block in range(factor.shape[0]):
        innovation = (factor[block : block + 1, :] * change).astype(bf16)
        cross_t = contract_lanes(innovation, scaled[block])
        weights_t = dot3(split(cross_t), split(inverse[block]))
        weights_out[block] = (weights_t * (1.0 / math.sqrt(members - 1.0))).astype(bf16)


def update_kernel(cells, weights_t, updated):
    blocks = weights_t.shape[0]
    width = cells.shape[1] // blocks
    for block in range(blocks):
        span = slice(block * width, (block + 1) * width)
        values = cells[:, span].astype(f32)
        centred = (values - jnp.mean(values, axis=0, keepdims=True)).astype(bf16)
        updated[:, span] = (values + dot(weights_t[block], centred)).astype(bf16)


def call(kernel, outs, flops, scalars=0):
    vmem = pl.BlockSpec(memory_space=pltpu.VMEM)
    smem = pl.BlockSpec(memory_space=pltpu.SMEM)

    def run(*args):
        return pl.pallas_call(
            kernel,
            out_shape=outs,
            in_specs=[smem] * scalars + [vmem] * (len(args) - scalars),
            out_specs=jax.tree.map(lambda _: vmem, outs),
            cost_estimate=pl.CostEstimate(flops=flops, transcendentals=0, bytes_accessed=1 << 22),
            name=kernel.__name__,
        )(*args)

    return run


def per_device(state, predicted, perturbed, obs_weight, obs_position, row_count, row_index):
    exchange = lambda value: lax.all_to_all(value, "member", split_axis=1, concat_axis=0, tiled=True)
    groups = lax.axis_size("member")
    group_index = lax.axis_index("member")
    tile_index = lax.axis_index("domain")
    blocks = row_index.shape[1]
    members = state.shape[0] * groups
    rows = predicted.shape[1] // groups

    pred_pool = exchange(predicted)
    pert_pool = exchange(perturbed)
    cells = exchange(state)

    counts = lax.dynamic_index_in_dim(row_count, tile_index, 0, keepdims=False)
    first_block = (tile_index * groups + group_index) * blocks
    scalars = jnp.concatenate([first_block[None].astype(jnp.int32), counts])
    weight = lax.dynamic_slice_in_dim(obs_weight, group_index * rows, rows)[None]
    place = lax.dynamic_slice_in_dim(obs_position, group_index * rows, rows)[None]

    shaped = jax.ShapeDtypeStruct
    cube = 2 * blocks * members**3
    factor = call(factor_kernel, shaped((blocks, rows), f32), cube // 4, 1)(scalars, row_index[0], weight, place)
    scaled, inverse = call(
        inverse_kernel,
        (shaped((blocks, members, rows), bf16), shaped((blocks, members, members), f32)),
        30 * cube,
    )(pred_pool, factor)
    weights_t = call(weights_kernel, shaped((blocks, members, members), bf16), 7 * cube)(
        pred_pool, pert_pool, factor, scaled, inverse
    )
    updated = call(update_kernel, shaped(cells.shape, bf16), cube)(cells, weights_t)
    return lax.all_to_all(updated, "member", split_axis=0, concat_axis=1, tiled=True)


def solution(mesh):
    placed = (
        P("member", "domain"),
        P("member", "domain"),
        P("member", "domain"),
        P("domain"),
        P("domain"),
        P(None, "member"),
        P("domain", "member", None),
    )
    return jax.shard_map(
        per_device, mesh=mesh, in_specs=placed, out_specs=P("member", "domain"), check_vma=False
    )
```

```python
import math

import jax
import jax.numpy as jnp
from jax import lax
from jax.experimental import pallas as pl
from jax.experimental.pallas import tpu as pltpu
from jax.sharding import PartitionSpec as P

NS_STEPS = 5
SPAN = 2
LANES = 128

f32 = jnp.float32
bf16 = jnp.bfloat16


def contract_lanes(left, right):
    return lax.dot_general(left, right, (((1,), (1,)), ((), ())), preferred_element_type=f32)


def contract_rows(left, right):
    return lax.dot_general(left, right, (((0,), (0,)), ((), ())), preferred_element_type=f32)


def dot(left, right):
    return jnp.dot(left, right, preferred_element_type=f32)


def split(value):
    high = value.astype(bf16)
    return high, (value - high.astype(f32)).astype(bf16)


def dot3(left, right):
    left_high, left_low = left
    right_high, right_low = right
    return dot(left_high, right_high) + (dot(left_high, right_low) + dot(left_low, right_high))


def factor_kernel(scalars, index, weight, place, factor_out):
    blocks, rows = index.shape
    tiles = rows // LANES
    for block in range(blocks):
        listed = index[block : block + 1, :]
        live = lax.broadcasted_iota(jnp.int32, (1, rows), 1) < scalars[1 + block]
        high = jnp.where(live, listed // LANES, -1)
        low = listed % LANES
        high_hot = (lax.broadcasted_iota(jnp.int32, (tiles, rows), 0) == high).astype(f32).astype(bf16)
        low_hot = (lax.broadcasted_iota(jnp.int32, (LANES, rows), 0) == low).astype(f32).astype(bf16)
        chosen = contract_lanes(high_hot, low_hot)
        chosen = jnp.concatenate([chosen[t : t + 1, :] for t in range(tiles)], axis=1)
        offset = (place[...] - (scalars[0] + block)).astype(f32) / SPAN
        taper = 1.0 / (1.0 + offset * offset)
        factor_out[block : block + 1, :] = jnp.where(chosen > 0.5, weight[...] * taper, 0.0)


def gain_kernel(first, factor, gain_out):
    members = first.shape[0]
    blocks, rows = factor.shape
    width = (first.shape[1] - rows) // blocks
    values = first[:, :rows].astype(f32)
    deviation = values - jnp.mean(values, axis=0, keepdims=True)
    eye = (
        lax.broadcasted_iota(jnp.int32, (members, members), 0)
        == lax.broadcasted_iota(jnp.int32, (members, members), 1)
    ).astype(f32)
    for block in range(blocks):
        scaled = (factor[block : block + 1, :] * deviation * (1.0 / math.sqrt(members - 1.0))).astype(bf16)
        gram = contract_lanes(scaled, scaled)
        start = 2.0 / (2.0 + jnp.sqrt(jnp.sum(gram * gram)))
        residual = eye - start * (eye + gram)
        estimate = eye + residual
        residual_parts = split(residual)
        for step in range(1, NS_STEPS):
            residual = dot3(residual_parts, residual_parts)
            residual_parts = split(residual)
            estimate = estimate + dot3(split(estimate), residual_parts)
        cells = first[:, rows + block * width : rows + (block + 1) * width].astype(f32)
        centred = (cells - jnp.mean(cells, axis=0, keepdims=True)).astype(bf16)
        high, low = split(estimate * (start * (1.0 / math.sqrt(members - 1.0))))
        smoothed_high, smoothed_low = split(dot(high, centred) + dot(low, centred))
        gain_out[block] = (
            contract_rows(scaled, smoothed_high) + contract_rows(scaled, smoothed_low)
        ).astype(bf16)


def update_kernel(first, pert, factor, gain, updated):
    blocks, rows = factor.shape
    width = (first.shape[1] - rows) // blocks
    change = pert[...].astype(f32) - first[:, :rows].astype(f32)
    for block in range(blocks):
        innovation = (factor[block : block + 1, :] * change).astype(bf16)
        cells = first[:, rows + block * width : rows + (block + 1) * width].astype(f32)
        updated[:, block * width : (block + 1) * width] = (cells + dot(innovation, gain[block])).astype(bf16)


def call(kernel, outs, flops, scalars=0):
    vmem = pl.BlockSpec(memory_space=pltpu.VMEM)
    smem = pl.BlockSpec(memory_space=pltpu.SMEM)

    def run(*args):
        return pl.pallas_call(
            kernel,
            out_shape=outs,
            in_specs=[smem] * scalars + [vmem] * (len(args) - scalars),
            out_specs=jax.tree.map(lambda _: vmem, outs),
            cost_estimate=pl.CostEstimate(flops=flops, transcendentals=0, bytes_accessed=1 << 22),
            name=kernel.__name__,
        )(*args)

    return run


def per_device(state, predicted, perturbed, obs_weight, obs_position, row_count, row_index):
    exchange = lambda value: lax.all_to_all(
        value.reshape(value.shape[0], groups, -1), "member", split_axis=1, concat_axis=0, tiled=True
    ).reshape(members, -1)
    groups = lax.axis_size("member")
    group_index = lax.axis_index("member")
    tile_index = lax.axis_index("domain")
    blocks = row_index.shape[1]
    held = state.shape[0]
    members = held * groups
    rows = predicted.shape[1] // groups
    cells = state.shape[1] // groups

    paired = jnp.concatenate(
        [predicted.reshape(held, groups, rows), state.reshape(held, groups, cells)], axis=2
    )
    first = exchange(paired)

    counts = lax.dynamic_index_in_dim(row_count, tile_index, 0, keepdims=False)
    first_block = (tile_index * groups + group_index) * blocks
    scalars = jnp.concatenate([first_block[None].astype(jnp.int32), counts])
    weight = lax.dynamic_slice_in_dim(obs_weight, group_index * rows, rows)[None]
    place = lax.dynamic_slice_in_dim(obs_position, group_index * rows, rows)[None]

    shaped = jax.ShapeDtypeStruct
    cube = 2 * blocks * members**3
    factor = call(factor_kernel, shaped((blocks, rows), f32), cube, 1)(scalars, row_index[0], weight, place)
    factor, perturbed = lax.optimization_barrier((factor, perturbed))
    pert_pool = exchange(perturbed)
    gain = call(gain_kernel, shaped((blocks, rows, cells // blocks), bf16), 40 * cube)(first, factor)
    updated = call(update_kernel, shaped((members, cells), bf16), 4 * cube)(first, pert_pool, factor, gain)
    return lax.all_to_all(updated, "member", split_axis=0, concat_axis=1, tiled=True)


def solution(mesh):
    placed = (
        P("member", "domain"),
        P("member", "domain"),
        P("member", "domain"),
        P("domain"),
        P("domain"),
        P(None, "member"),
        P("domain", "member", None),
    )
    return jax.shard_map(
        per_device, mesh=mesh, in_specs=placed, out_specs=P("member", "domain"), check_vma=False
    )
```

```python
import math

import jax
import jax.numpy as jnp
from jax import lax
from jax.experimental import pallas as pl
from jax.experimental.pallas import tpu as pltpu
from jax.sharding import PartitionSpec as P

NS_STEPS = 5
SPAN = 2
LANES = 128
PIECES = 4

f32 = jnp.float32
bf16 = jnp.bfloat16


def contract_lanes(left, right):
    return lax.dot_general(left, right, (((1,), (1,)), ((), ())), preferred_element_type=f32)


def contract_rows(left, right):
    return lax.dot_general(left, right, (((0,), (0,)), ((), ())), preferred_element_type=f32)


def dot(left, right):
    return jnp.dot(left, right, preferred_element_type=f32)


def split(value):
    high = value.astype(bf16)
    return high, (value - high.astype(f32)).astype(bf16)


def dot3(left, right):
    left_high, left_low = left
    right_high, right_low = right
    return dot(left_high, right_high) + (dot(left_high, right_low) + dot(left_low, right_high))


def factor_kernel(scalars, index, weight, place, factor_out):
    blocks, rows = index.shape
    tiles = rows // LANES
    for block in range(blocks):
        listed = index[block : block + 1, :]
        live = lax.broadcasted_iota(jnp.int32, (1, rows), 1) < scalars[1 + block]
        high = jnp.where(live, listed // LANES, -1)
        low = listed % LANES
        high_hot = (lax.broadcasted_iota(jnp.int32, (tiles, rows), 0) == high).astype(f32).astype(bf16)
        low_hot = (lax.broadcasted_iota(jnp.int32, (LANES, rows), 0) == low).astype(f32).astype(bf16)
        chosen = contract_lanes(high_hot, low_hot)
        chosen = jnp.concatenate([chosen[t : t + 1, :] for t in range(tiles)], axis=1)
        offset = (place[...] - (scalars[0] + block)).astype(f32) / SPAN
        taper = 1.0 / (1.0 + offset * offset)
        factor_out[block : block + 1, :] = jnp.where(chosen > 0.5, weight[...] * taper, 0.0)


def gain_kernel(pred, factor, gain_out, pred_buf, sem):
    members, rows = pred.shape
    load = pltpu.make_async_copy(pred, pred_buf, sem)
    load.start()
    load.wait()
    values = pred_buf[...].astype(f32)
    deviation = values - jnp.mean(values, axis=0, keepdims=True)
    eye = (
        lax.broadcasted_iota(jnp.int32, (members, members), 0)
        == lax.broadcasted_iota(jnp.int32, (members, members), 1)
    ).astype(f32)
    for block in range(factor.shape[0]):
        scaled = (factor[block : block + 1, :] * deviation * (1.0 / math.sqrt(members - 1.0))).astype(bf16)
        gram = contract_lanes(scaled, scaled)
        start = 2.0 / (2.0 + jnp.sqrt(jnp.sum(gram * gram)))
        residual = eye - start * (eye + gram)
        estimate = eye + residual
        residual_parts = split(residual)
        for step in range(1, NS_STEPS):
            residual = dot3(residual_parts, residual_parts)
            residual_parts = split(residual)
            estimate = estimate + dot3(split(estimate), residual_parts)
        high, low = split(estimate * (start * (1.0 / math.sqrt(members - 1.0))))
        gain_out[:, block * members : (block + 1) * members] = (contract_rows(scaled, high) + contract_rows(scaled, low)).astype(bf16)


def update_kernel(second, factor, pred, gain, updated, pred_buf, gain_buf, pred_sems, gain_sems):
    blocks, rows = factor.shape
    members = pred.shape[0]
    width = (second.shape[1] - rows) // blocks
    piece = rows // PIECES
    pred_loads, gain_loads = [], []
    for part in range(PIECES):
        span = pl.ds(part * piece, piece)
        pred_loads.append(pltpu.make_async_copy(pred.at[:, span], pred_buf.at[:, span], pred_sems.at[part]))
        gain_loads.append(pltpu.make_async_copy(gain.at[span, :], gain_buf.at[span, :], gain_sems.at[part]))
        pred_loads[part].start()
        gain_loads[part].start()
    weights_t = [None] * blocks
    for part in range(PIECES):
        span = slice(part * piece, (part + 1) * piece)
        pred_loads[part].wait()
        change = second[:, span].astype(f32) - pred_buf[:, span].astype(f32)
        gain_loads[part].wait()
        for block in range(blocks):
            innovation = (factor[block : block + 1, span] * change).astype(bf16)
            product = dot(innovation, gain_buf[span, block * members : (block + 1) * members])
            weights_t[block] = product if part == 0 else weights_t[block] + product
    for block in range(blocks):
        span = slice(rows + block * width, rows + (block + 1) * width)
        cells = second[:, span].astype(f32)
        centred = (cells - jnp.mean(cells, axis=0, keepdims=True)).astype(bf16)
        change = dot(weights_t[block].astype(bf16), centred)
        updated[:, block * width : (block + 1) * width] = (cells + change).astype(bf16)


def call(kernel, outs, flops, grant=None, scalars=0, stay=(), scratch=()):
    vmem = pl.BlockSpec(memory_space=pltpu.VMEM)
    smem = pl.BlockSpec(memory_space=pltpu.SMEM)
    hbm = pl.BlockSpec(memory_space=pltpu.HBM)

    def run(*args):
        specs = [smem] * scalars + [vmem] * (len(args) - scalars)
        for place in stay:
            specs[place] = hbm
        args = [
            pltpu.with_memory_space_constraint(arg, pltpu.HBM) if place in stay else arg
            for place, arg in enumerate(args)
        ]
        return pl.pallas_call(
            kernel,
            out_shape=outs,
            in_specs=specs,
            out_specs=vmem,
            scratch_shapes=list(scratch),
            cost_estimate=pl.CostEstimate(flops=flops, transcendentals=0, bytes_accessed=1 << 22),
            compiler_params=pltpu.CompilerParams(vmem_limit_bytes=grant),
            name=kernel.__name__,
        )(*args)

    return run


def per_device(state, predicted, perturbed, obs_weight, obs_position, row_count, row_index):
    exchange = lambda value: lax.all_to_all(
        value.reshape(value.shape[0], groups, -1), "member", split_axis=1, concat_axis=0, tiled=True
    ).reshape(members, -1)
    groups = lax.axis_size("member")
    group_index = lax.axis_index("member")
    tile_index = lax.axis_index("domain")
    blocks = row_index.shape[1]
    held = state.shape[0]
    members = held * groups
    rows = predicted.shape[1] // groups
    cells = state.shape[1] // groups

    pred_pool = exchange(predicted)
    counts = lax.dynamic_index_in_dim(row_count, tile_index, 0, keepdims=False)
    first_block = (tile_index * groups + group_index) * blocks
    scalars = jnp.concatenate([first_block[None].astype(jnp.int32), counts])
    weight = lax.dynamic_slice_in_dim(obs_weight, group_index * rows, rows)[None]
    place = lax.dynamic_slice_in_dim(obs_position, group_index * rows, rows)[None]

    shaped = jax.ShapeDtypeStruct
    cube = 2 * blocks * members**3
    factor = call(factor_kernel, shaped((blocks, rows), f32), cube, 67043328, 1)(scalars, row_index[0], weight, place)
    paired = jnp.concatenate(
        [perturbed.reshape(held, groups, rows), state.reshape(held, groups, cells)], axis=2
    )
    factor, paired = lax.optimization_barrier((factor, paired))
    second = exchange(paired)
    gain = call(
        gain_kernel,
        shaped((rows, blocks * members), bf16),
        40 * cube,
        stay=(0,),
        scratch=(pltpu.VMEM((members, rows), bf16), pltpu.SemaphoreType.DMA),
    )(pred_pool, factor)
    updated = call(
        update_kernel,
        shaped((members, cells), bf16),
        5 * cube,
        grant=24 << 20,
        stay=(2, 3),
        scratch=(
            pltpu.VMEM((members, rows), bf16),
            pltpu.VMEM(gain.shape, bf16),
            pltpu.SemaphoreType.DMA((PIECES,)),
            pltpu.SemaphoreType.DMA((PIECES,)),
        ),
    )(second, factor, pred_pool, gain)
    return lax.all_to_all(updated, "member", split_axis=0, concat_axis=1, tiled=True)


def solution(mesh):
    placed = (
        P("member", "domain"),
        P("member", "domain"),
        P("member", "domain"),
        P("domain"),
        P("domain"),
        P(None, "member"),
        P("domain", "member", None),
    )
    return jax.shard_map(
        per_device, mesh=mesh, in_specs=placed, out_specs=P("member", "domain"), check_vma=False
    )
```

```python
import math

import jax
import jax.numpy as jnp
from jax import lax
from jax.experimental import pallas as pl
from jax.experimental.pallas import tpu as pltpu
from jax.sharding import PartitionSpec as P

NS_STEPS = 5
SPAN = 2
LANES = 128
PIECES = 4
HELD = 8

f32 = jnp.float32
bf16 = jnp.bfloat16


def contract_lanes(left, right):
    return lax.dot_general(left, right, (((1,), (1,)), ((), ())), preferred_element_type=f32)


def contract_rows(left, right):
    return lax.dot_general(left, right, (((0,), (0,)), ((), ())), preferred_element_type=f32)


def dot(left, right):
    return jnp.dot(left, right, preferred_element_type=f32)


def split(value):
    high = value.astype(bf16)
    return high, (value - high.astype(f32)).astype(bf16)


def dot3(left, right):
    left_high, left_low = left
    right_high, right_low = right
    return dot(left_high, right_high) + (dot(left_high, right_low) + dot(left_low, right_high))


def factor_kernel(scalars, index, weight, place, factor_out):
    blocks, rows = index.shape
    tiles = rows // LANES
    for block in range(blocks):
        listed = index[block : block + 1, :]
        live = lax.broadcasted_iota(jnp.int32, (1, rows), 1) < scalars[1 + block]
        high = jnp.where(live, listed // LANES, -1)
        low = listed % LANES
        high_hot = (lax.broadcasted_iota(jnp.int32, (tiles, rows), 0) == high).astype(f32).astype(bf16)
        low_hot = (lax.broadcasted_iota(jnp.int32, (LANES, rows), 0) == low).astype(f32).astype(bf16)
        chosen = contract_lanes(high_hot, low_hot)
        chosen = jnp.concatenate([chosen[t : t + 1, :] for t in range(tiles)], axis=1)
        offset = (place[...] - (scalars[0] + block)).astype(f32) / SPAN
        taper = 1.0 / (1.0 + offset * offset)
        factor_out[block : block + 1, :] = jnp.where(chosen > 0.5, weight[...] * taper, 0.0)


def gain_kernel(pred, factor, gain_out, pred_buf, sem):
    members, rows = pred.shape
    load = pltpu.make_async_copy(pred, pred_buf, sem)
    load.start()
    load.wait()
    values = pred_buf[...].astype(f32)
    deviation = values - jnp.mean(values, axis=0, keepdims=True)
    eye = (
        lax.broadcasted_iota(jnp.int32, (members, members), 0)
        == lax.broadcasted_iota(jnp.int32, (members, members), 1)
    ).astype(f32)
    for block in range(factor.shape[0]):
        scaled = (factor[block : block + 1, :] * deviation * (1.0 / math.sqrt(members - 1.0))).astype(bf16)
        gram = contract_lanes(scaled, scaled)
        start = 2.0 / (2.0 + jnp.sqrt(jnp.sum(gram * gram)))
        residual = eye - start * (eye + gram)
        estimate = eye + residual
        residual_parts = split(residual)
        for step in range(1, NS_STEPS):
            residual = dot3(residual_parts, residual_parts)
            residual_parts = split(residual)
            estimate = estimate + dot3(split(estimate), residual_parts)
        high, low = split(estimate * (start * (1.0 / math.sqrt(members - 1.0))))
        gain_out[:, block * members : (block + 1) * members] = (contract_rows(scaled, high) + contract_rows(scaled, low)).astype(bf16)


def update_kernel(second, factor, pred, gain, updated, pred_buf, gain_buf, pred_sems, gain_sems):
    blocks, rows = factor.shape
    members = pred.shape[0]
    width = (second.shape[1] - rows) // blocks
    piece = rows // PIECES
    pred_loads, gain_loads = [], []
    for part in range(PIECES):
        span = pl.ds(part * piece, piece)
        pred_loads.append(pltpu.make_async_copy(pred.at[:, span], pred_buf.at[:, span], pred_sems.at[part]))
        gain_loads.append(pltpu.make_async_copy(gain.at[span, :], gain_buf.at[span, :], gain_sems.at[part]))
        pred_loads[part].start()
        gain_loads[part].start()
    weights_t = [None] * blocks
    for part in range(PIECES):
        span = slice(part * piece, (part + 1) * piece)
        pred_loads[part].wait()
        change = second[:, span].astype(f32) - pred_buf[:, span].astype(f32)
        gain_loads[part].wait()
        for block in range(blocks):
            innovation = (factor[block : block + 1, span] * change).astype(bf16)
            product = dot(innovation, gain_buf[span, block * members : (block + 1) * members])
            weights_t[block] = product if part == 0 else weights_t[block] + product
    for block in range(blocks):
        span = slice(rows + block * width, rows + (block + 1) * width)
        cells = second[:, span].astype(f32)
        centred = (cells - jnp.mean(cells, axis=0, keepdims=True)).astype(bf16)
        total = cells + dot(weights_t[block].astype(bf16), centred)
        total = jnp.concatenate([total[row : row + HELD] for row in range(members - HELD, -1, -HELD)], axis=0)
        updated[:, block * width : (block + 1) * width] = total.astype(bf16)


def call(kernel, outs, flops, grant=None, scalars=0, stay=(), scratch=()):
    vmem = pl.BlockSpec(memory_space=pltpu.VMEM)
    smem = pl.BlockSpec(memory_space=pltpu.SMEM)
    hbm = pl.BlockSpec(memory_space=pltpu.HBM)

    def run(*args):
        specs = [smem] * scalars + [vmem] * (len(args) - scalars)
        for place in stay:
            specs[place] = hbm
        args = [
            pltpu.with_memory_space_constraint(arg, pltpu.HBM) if place in stay else arg
            for place, arg in enumerate(args)
        ]
        return pl.pallas_call(
            kernel,
            out_shape=outs,
            in_specs=specs,
            out_specs=vmem,
            scratch_shapes=list(scratch),
            cost_estimate=pl.CostEstimate(flops=flops, transcendentals=0, bytes_accessed=1 << 22),
            compiler_params=pltpu.CompilerParams(vmem_limit_bytes=grant),
            name=kernel.__name__,
        )(*args)

    return run


def per_device(state, predicted, perturbed, obs_weight, obs_position, row_count, row_index):
    exchange = lambda value: lax.all_to_all(
        value.reshape(value.shape[0], groups, -1), "member", split_axis=1, concat_axis=0, tiled=True
    ).reshape(members, -1)
    groups = lax.axis_size("member")
    group_index = lax.axis_index("member")
    tile_index = lax.axis_index("domain")
    blocks = row_index.shape[1]
    held = state.shape[0]
    members = held * groups
    rows = predicted.shape[1] // groups
    cells = state.shape[1] // groups

    pred_pool = exchange(predicted)
    counts = lax.dynamic_index_in_dim(row_count, tile_index, 0, keepdims=False)
    first_block = (tile_index * groups + group_index) * blocks
    scalars = jnp.concatenate([first_block[None].astype(jnp.int32), counts])
    weight = lax.dynamic_slice_in_dim(obs_weight, group_index * rows, rows)[None]
    place = lax.dynamic_slice_in_dim(obs_position, group_index * rows, rows)[None]

    shaped = jax.ShapeDtypeStruct
    cube = 2 * blocks * members**3
    factor = call(factor_kernel, shaped((blocks, rows), f32), cube, 67043328, 1)(scalars, row_index[0], weight, place)
    paired = jnp.concatenate(
        [perturbed.reshape(held, groups, rows), state.reshape(held, groups, cells)], axis=2
    )
    factor, paired = lax.optimization_barrier((factor, paired))
    second = exchange(paired)
    gain = call(
        gain_kernel,
        shaped((rows, blocks * members), bf16),
        40 * cube,
        stay=(0,),
        scratch=(pltpu.VMEM((members, rows), bf16), pltpu.SemaphoreType.DMA),
    )(pred_pool, factor)
    updated = call(
        update_kernel,
        shaped((members, cells), bf16),
        5 * cube,
        grant=24 << 20,
        stay=(2, 3),
        scratch=(
            pltpu.VMEM((members, rows), bf16),
            pltpu.VMEM(gain.shape, bf16),
            pltpu.SemaphoreType.DMA((PIECES,)),
            pltpu.SemaphoreType.DMA((PIECES,)),
        ),
    )(second, factor, pred_pool, gain)
    backwards = [list(range(groups))[::-1]]
    returned = lax.all_to_all(
        updated, "member", split_axis=0, concat_axis=1, tiled=True, axis_index_groups=backwards
    )
    return jnp.flip(returned.reshape(held, groups, cells), axis=1).reshape(held, -1)


def solution(mesh):
    placed = (
        P("member", "domain"),
        P("member", "domain"),
        P("member", "domain"),
        P("domain"),
        P("domain"),
        P(None, "member"),
        P("domain", "member", None),
    )
    return jax.shard_map(
        per_device, mesh=mesh, in_specs=placed, out_specs=P("member", "domain"), check_vma=False
    )
```

```python
import math

import jax
import jax.numpy as jnp
from jax import lax
from jax.experimental import pallas as pl
from jax.experimental.pallas import tpu as pltpu
from jax.sharding import PartitionSpec as P

NS_STEPS = 5
SPAN = 2
LANES = 128
PIECES = 4
HELD = 8

f32 = jnp.float32
bf16 = jnp.bfloat16


def contract_lanes(left, right):
    return lax.dot_general(left, right, (((1,), (1,)), ((), ())), preferred_element_type=f32)


def contract_rows(left, right):
    return lax.dot_general(left, right, (((0,), (0,)), ((), ())), preferred_element_type=f32)


def dot(left, right):
    return jnp.dot(left, right, preferred_element_type=f32)


def split(value):
    high = value.astype(bf16)
    return high, (value - high.astype(f32)).astype(bf16)


def dot3(left, right):
    left_high, left_low = left
    right_high, right_low = right
    return dot(left_high, right_high) + (dot(left_high, right_low) + dot(left_low, right_high))


def backwards(value):
    last = value.shape[0] - HELD
    return jnp.concatenate([value[row : row + HELD] for row in range(last, -1, -HELD)], axis=0)


def factor_kernel(scalars, index, weight, place, factor_out):
    blocks, rows = index.shape
    tiles = rows // LANES
    for block in range(blocks):
        listed = index[block : block + 1, :]
        live = lax.broadcasted_iota(jnp.int32, (1, rows), 1) < scalars[1 + block]
        high = jnp.where(live, listed // LANES, -1)
        low = listed % LANES
        high_hot = (lax.broadcasted_iota(jnp.int32, (tiles, rows), 0) == high).astype(f32).astype(bf16)
        low_hot = (lax.broadcasted_iota(jnp.int32, (LANES, rows), 0) == low).astype(f32).astype(bf16)
        chosen = contract_lanes(high_hot, low_hot)
        chosen = jnp.concatenate([chosen[t : t + 1, :] for t in range(tiles)], axis=1)
        offset = (place[...] - (scalars[0] + block)).astype(f32) / SPAN
        taper = 1.0 / (1.0 + offset * offset)
        factor_out[block : block + 1, :] = jnp.where(chosen > 0.5, weight[...] * taper, 0.0)


def gain_kernel(pred, factor, gain_out, pred_buf, sem):
    members, rows = pred.shape
    load = pltpu.make_async_copy(pred, pred_buf, sem)
    load.start()
    load.wait()
    values = backwards(pred_buf[...].astype(f32))
    deviation = values - jnp.mean(values, axis=0, keepdims=True)
    eye = (
        lax.broadcasted_iota(jnp.int32, (members, members), 0)
        == lax.broadcasted_iota(jnp.int32, (members, members), 1)
    ).astype(f32)
    for block in range(factor.shape[0]):
        scaled = (factor[block : block + 1, :] * deviation * (1.0 / math.sqrt(members - 1.0))).astype(bf16)
        gram = contract_lanes(scaled, scaled)
        start = 2.0 / (2.0 + jnp.sqrt(jnp.sum(gram * gram)))
        residual = eye - start * (eye + gram)
        estimate = eye + residual
        residual_parts = split(residual)
        for step in range(1, NS_STEPS):
            residual = dot3(residual_parts, residual_parts)
            residual_parts = split(residual)
            estimate = estimate + dot3(split(estimate), residual_parts)
        high, low = split(estimate * (start * (1.0 / math.sqrt(members - 1.0))))
        gain_out[:, block * members : (block + 1) * members] = (contract_rows(scaled, high) + contract_rows(scaled, low)).astype(bf16)


def update_kernel(second, factor, pred, gain, updated, pred_buf, gain_buf, pred_sems, gain_sems):
    blocks, rows = factor.shape
    members = pred.shape[0]
    width = (second.shape[1] - rows) // blocks
    piece = rows // PIECES
    pred_loads, gain_loads = [], []
    for part in range(PIECES):
        span = pl.ds(part * piece, piece)
        pred_loads.append(pltpu.make_async_copy(pred.at[:, span], pred_buf.at[:, span], pred_sems.at[part]))
        gain_loads.append(pltpu.make_async_copy(gain.at[span, :], gain_buf.at[span, :], gain_sems.at[part]))
        pred_loads[part].start()
        gain_loads[part].start()
    weights_t = [None] * blocks
    for part in range(PIECES):
        span = slice(part * piece, (part + 1) * piece)
        pred_loads[part].wait()
        change = second[:, span].astype(f32) - backwards(pred_buf[:, span].astype(f32))
        gain_loads[part].wait()
        for block in range(blocks):
            innovation = (factor[block : block + 1, span] * change).astype(bf16)
            product = dot(innovation, gain_buf[span, block * members : (block + 1) * members])
            weights_t[block] = product if part == 0 else weights_t[block] + product
    for block in range(blocks):
        span = slice(rows + block * width, rows + (block + 1) * width)
        cells = second[:, span].astype(f32)
        centred = (cells - jnp.mean(cells, axis=0, keepdims=True)).astype(bf16)
        change = dot(weights_t[block].astype(bf16), centred)
        updated[:, block * width : (block + 1) * width] = (cells + change).astype(bf16)


def call(kernel, outs, flops, grant=None, scalars=0, stay=(), scratch=()):
    vmem = pl.BlockSpec(memory_space=pltpu.VMEM)
    smem = pl.BlockSpec(memory_space=pltpu.SMEM)
    hbm = pl.BlockSpec(memory_space=pltpu.HBM)

    def run(*args):
        specs = [smem] * scalars + [vmem] * (len(args) - scalars)
        for place in stay:
            specs[place] = hbm
        args = [
            pltpu.with_memory_space_constraint(arg, pltpu.HBM) if place in stay else arg
            for place, arg in enumerate(args)
        ]
        return pl.pallas_call(
            kernel,
            out_shape=outs,
            in_specs=specs,
            out_specs=vmem,
            scratch_shapes=list(scratch),
            cost_estimate=pl.CostEstimate(flops=flops, transcendentals=0, bytes_accessed=1 << 22),
            compiler_params=pltpu.CompilerParams(vmem_limit_bytes=grant),
            name=kernel.__name__,
        )(*args)

    return run


def per_device(state, predicted, perturbed, obs_weight, obs_position, row_count, row_index):
    def exchange(value, order=None):
        chunks = value.reshape(held, groups, -1)
        received = lax.all_to_all(
            chunks, "member", split_axis=1, concat_axis=0, tiled=True, axis_index_groups=order
        )
        return received.reshape(members, -1)

    groups = lax.axis_size("member")
    group_index = lax.axis_index("member")
    tile_index = lax.axis_index("domain")
    blocks = row_index.shape[1]
    held = state.shape[0]
    members = held * groups
    rows = predicted.shape[1] // groups
    cells = state.shape[1] // groups
    from_last = [list(range(groups))[::-1]]

    pred_pool = exchange(predicted)
    counts = lax.dynamic_index_in_dim(row_count, tile_index, 0, keepdims=False)
    first_block = (tile_index * groups + group_index) * blocks
    scalars = jnp.concatenate([first_block[None].astype(jnp.int32), counts])
    weight = lax.dynamic_slice_in_dim(obs_weight, group_index * rows, rows)[None]
    place = lax.dynamic_slice_in_dim(obs_position, group_index * rows, rows)[None]

    shaped = jax.ShapeDtypeStruct
    cube = 2 * blocks * members**3
    factor = call(factor_kernel, shaped((blocks, rows), f32), cube, 67043328, 1)(scalars, row_index[0], weight, place)
    paired = jnp.concatenate(
        [perturbed.reshape(held, groups, rows), state.reshape(held, groups, cells)], axis=2
    )
    factor, paired = lax.optimization_barrier((factor, jnp.flip(paired, axis=1)))
    second = exchange(paired, from_last)
    gain = call(
        gain_kernel,
        shaped((rows, blocks * members), bf16),
        40 * cube,
        stay=(0,),
        scratch=(pltpu.VMEM((members, rows), bf16), pltpu.SemaphoreType.DMA),
    )(pred_pool, factor)
    updated = call(
        update_kernel,
        shaped((members, cells), bf16),
        5 * cube,
        grant=24 << 20,
        stay=(2, 3),
        scratch=(
            pltpu.VMEM((members, rows), bf16),
            pltpu.VMEM(gain.shape, bf16),
            pltpu.SemaphoreType.DMA((PIECES,)),
            pltpu.SemaphoreType.DMA((PIECES,)),
        ),
    )(second, factor, pred_pool, gain)
    returned = lax.all_to_all(
        updated, "member", split_axis=0, concat_axis=1, tiled=True, axis_index_groups=from_last
    )
    return jnp.flip(returned.reshape(held, groups, cells), axis=1).reshape(held, -1)


def solution(mesh):
    placed = (
        P("member", "domain"),
        P("member", "domain"),
        P("member", "domain"),
        P("domain"),
        P("domain"),
        P(None, "member"),
        P("domain", "member", None),
    )
    return jax.shard_map(
        per_device, mesh=mesh, in_specs=placed, out_specs=P("member", "domain"), check_vma=False
    )
```

```python
import math

import jax
import jax.numpy as jnp
from jax import lax
from jax.experimental import pallas as pl
from jax.experimental.pallas import tpu as pltpu
from jax.sharding import PartitionSpec as P

NS_STEPS = 5
SPAN = 2
LANES = 128
PIECES = 4
HELD = 8

f32 = jnp.float32
bf16 = jnp.bfloat16


def contract_lanes(left, right):
    return lax.dot_general(left, right, (((1,), (1,)), ((), ())), preferred_element_type=f32)


def contract_rows(left, right):
    return lax.dot_general(left, right, (((0,), (0,)), ((), ())), preferred_element_type=f32)


def dot(left, right):
    return jnp.dot(left, right, preferred_element_type=f32)


def split(value):
    high = value.astype(bf16)
    return high, (value - high.astype(f32)).astype(bf16)


def dot3(left, right):
    left_high, left_low = left
    right_high, right_low = right
    return dot(left_high, right_high) + (dot(left_high, right_low) + dot(left_low, right_high))


def backwards(value):
    last = value.shape[0] - HELD
    return jnp.concatenate([value[row : row + HELD] for row in range(last, -1, -HELD)], axis=0)


def from_middle(value):
    groups = value.shape[0] // HELD
    order = [groups - 1 - (groups // 2 + spot) % groups for spot in range(groups)]
    return jnp.concatenate([value[spot * HELD : (spot + 1) * HELD] for spot in order], axis=0)


def factor_kernel(scalars, index, weight, place, factor_out):
    blocks, rows = index.shape
    tiles = rows // LANES
    for block in range(blocks):
        listed = index[block : block + 1, :]
        live = lax.broadcasted_iota(jnp.int32, (1, rows), 1) < scalars[1 + block]
        high = jnp.where(live, listed // LANES, -1)
        low = listed % LANES
        high_hot = (lax.broadcasted_iota(jnp.int32, (tiles, rows), 0) == high).astype(f32).astype(bf16)
        low_hot = (lax.broadcasted_iota(jnp.int32, (LANES, rows), 0) == low).astype(f32).astype(bf16)
        chosen = contract_lanes(high_hot, low_hot)
        chosen = jnp.concatenate([chosen[t : t + 1, :] for t in range(tiles)], axis=1)
        offset = (place[...] - (scalars[0] + block)).astype(f32) / SPAN
        taper = 1.0 / (1.0 + offset * offset)
        factor_out[block : block + 1, :] = jnp.where(chosen > 0.5, weight[...] * taper, 0.0)


def gain_kernel(pred, factor, gain_out, pred_buf, sem):
    members, rows = pred.shape
    load = pltpu.make_async_copy(pred, pred_buf, sem)
    load.start()
    load.wait()
    values = backwards(pred_buf[...].astype(f32))
    deviation = values - jnp.mean(values, axis=0, keepdims=True)
    eye = (
        lax.broadcasted_iota(jnp.int32, (members, members), 0)
        == lax.broadcasted_iota(jnp.int32, (members, members), 1)
    ).astype(f32)
    for block in range(factor.shape[0]):
        scaled = (factor[block : block + 1, :] * deviation * (1.0 / math.sqrt(members - 1.0))).astype(bf16)
        gram = contract_lanes(scaled, scaled)
        start = 2.0 / (2.0 + jnp.sqrt(jnp.sum(gram * gram)))
        residual = eye - start * (eye + gram)
        estimate = eye + residual
        residual_parts = split(residual)
        for step in range(1, NS_STEPS):
            residual = dot3(residual_parts, residual_parts)
            residual_parts = split(residual)
            estimate = estimate + dot3(split(estimate), residual_parts)
        high, low = split(estimate * (start * (1.0 / math.sqrt(members - 1.0))))
        gain_out[:, block * members : (block + 1) * members] = (contract_rows(scaled, high) + contract_rows(scaled, low)).astype(bf16)


def update_kernel(second, factor, pred, gain, updated, pred_buf, gain_buf, pred_sems, gain_sems):
    blocks, rows = factor.shape
    members = pred.shape[0]
    width = (second.shape[1] - rows) // blocks
    piece = rows // PIECES
    pred_loads, gain_loads = [], []
    for part in range(PIECES):
        span = pl.ds(part * piece, piece)
        pred_loads.append(pltpu.make_async_copy(pred.at[:, span], pred_buf.at[:, span], pred_sems.at[part]))
        gain_loads.append(pltpu.make_async_copy(gain.at[span, :], gain_buf.at[span, :], gain_sems.at[part]))
        pred_loads[part].start()
        gain_loads[part].start()
    weights_t = [None] * blocks
    for part in range(PIECES):
        span = slice(part * piece, (part + 1) * piece)
        pred_loads[part].wait()
        change = second[:, span].astype(f32) - backwards(pred_buf[:, span].astype(f32))
        gain_loads[part].wait()
        for block in range(blocks):
            innovation = (factor[block : block + 1, span] * change).astype(bf16)
            product = dot(innovation, gain_buf[span, block * members : (block + 1) * members])
            weights_t[block] = product if part == 0 else weights_t[block] + product
    for block in range(blocks):
        span = slice(rows + block * width, rows + (block + 1) * width)
        cells = second[:, span].astype(f32)
        centred = (cells - jnp.mean(cells, axis=0, keepdims=True)).astype(bf16)
        total = from_middle(cells + dot(weights_t[block].astype(bf16), centred))
        updated[:, block * width : (block + 1) * width] = total.astype(bf16)


def call(kernel, outs, flops, grant=None, scalars=0, stay=(), scratch=()):
    vmem = pl.BlockSpec(memory_space=pltpu.VMEM)
    smem = pl.BlockSpec(memory_space=pltpu.SMEM)
    hbm = pl.BlockSpec(memory_space=pltpu.HBM)

    def run(*args):
        specs = [smem] * scalars + [vmem] * (len(args) - scalars)
        for place in stay:
            specs[place] = hbm
        args = [
            pltpu.with_memory_space_constraint(arg, pltpu.HBM) if place in stay else arg
            for place, arg in enumerate(args)
        ]
        return pl.pallas_call(
            kernel,
            out_shape=outs,
            in_specs=specs,
            out_specs=vmem,
            scratch_shapes=list(scratch),
            cost_estimate=pl.CostEstimate(flops=flops, transcendentals=0, bytes_accessed=1 << 22),
            compiler_params=pltpu.CompilerParams(vmem_limit_bytes=grant),
            name=kernel.__name__,
        )(*args)

    return run


def per_device(state, predicted, perturbed, obs_weight, obs_position, row_count, row_index):
    def exchange(value, order=None):
        chunks = value.reshape(held, groups, -1)
        received = lax.all_to_all(
            chunks, "member", split_axis=1, concat_axis=0, tiled=True, axis_index_groups=order
        )
        return received.reshape(members, -1)

    groups = lax.axis_size("member")
    group_index = lax.axis_index("member")
    tile_index = lax.axis_index("domain")
    blocks = row_index.shape[1]
    held = state.shape[0]
    members = held * groups
    rows = predicted.shape[1] // groups
    cells = state.shape[1] // groups
    from_last = [list(range(groups))[::-1]]

    pred_pool = exchange(predicted)
    counts = lax.dynamic_index_in_dim(row_count, tile_index, 0, keepdims=False)
    first_block = (tile_index * groups + group_index) * blocks
    scalars = jnp.concatenate([first_block[None].astype(jnp.int32), counts])
    weight = lax.dynamic_slice_in_dim(obs_weight, group_index * rows, rows)[None]
    place = lax.dynamic_slice_in_dim(obs_position, group_index * rows, rows)[None]

    shaped = jax.ShapeDtypeStruct
    cube = 2 * blocks * members**3
    factor = call(factor_kernel, shaped((blocks, rows), f32), cube, 67043328, 1)(scalars, row_index[0], weight, place)
    paired = jnp.concatenate(
        [perturbed.reshape(held, groups, rows), state.reshape(held, groups, cells)], axis=2
    )
    factor, paired = lax.optimization_barrier((factor, jnp.flip(paired, axis=1)))
    second = exchange(paired, from_last)
    gain = call(
        gain_kernel,
        shaped((rows, blocks * members), bf16),
        40 * cube,
        stay=(0,),
        scratch=(pltpu.VMEM((members, rows), bf16), pltpu.SemaphoreType.DMA),
    )(pred_pool, factor)
    updated = call(
        update_kernel,
        shaped((members, cells), bf16),
        5 * cube,
        grant=24 << 20,
        stay=(2, 3),
        scratch=(
            pltpu.VMEM((members, rows), bf16),
            pltpu.VMEM(gain.shape, bf16),
            pltpu.SemaphoreType.DMA((PIECES,)),
            pltpu.SemaphoreType.DMA((PIECES,)),
        ),
    )(second, factor, pred_pool, gain)
    half = groups // 2
    middle_first = [[(half + spot) % groups for spot in range(groups)]]
    returned = lax.all_to_all(
        updated, "member", split_axis=0, concat_axis=1, tiled=True, axis_index_groups=middle_first
    )
    return jnp.flip(returned.reshape(held, 2, half * cells), axis=1).reshape(held, -1)


def solution(mesh):
    placed = (
        P("member", "domain"),
        P("member", "domain"),
        P("member", "domain"),
        P("domain"),
        P("domain"),
        P(None, "member"),
        P("domain", "member", None),
    )
    return jax.shard_map(
        per_device, mesh=mesh, in_specs=placed, out_specs=P("member", "domain"), check_vma=False
    )
```

```python
import math

import jax
import jax.numpy as jnp
from jax import lax
from jax.experimental import pallas as pl
from jax.experimental.pallas import tpu as pltpu
from jax.sharding import PartitionSpec as P

NS_STEPS = 5
SPAN = 2
LANES = 128
PIECES = 4
HELD = 8

f32 = jnp.float32
bf16 = jnp.bfloat16


def contract_lanes(left, right):
    return lax.dot_general(left, right, (((1,), (1,)), ((), ())), preferred_element_type=f32)


def contract_rows(left, right):
    return lax.dot_general(left, right, (((0,), (0,)), ((), ())), preferred_element_type=f32)


def dot(left, right):
    return jnp.dot(left, right, preferred_element_type=f32)


def split(value):
    high = value.astype(bf16)
    return high, (value - high.astype(f32)).astype(bf16)


def dot3(left, right):
    left_high, left_low = left
    right_high, right_low = right
    return dot(left_high, right_high) + (dot(left_high, right_low) + dot(left_low, right_high))


def from_middle(value):
    half = value.shape[0] // 2
    return jnp.concatenate([value[half:], value[:half]], axis=0)


def from_last(value):
    groups = value.shape[0] // HELD
    order = [(groups // 2 - 1 - spot) % groups for spot in range(groups)]
    return jnp.concatenate([value[spot * HELD : (spot + 1) * HELD] for spot in order], axis=0)


def factor_kernel(scalars, index, weight, place, factor_out):
    blocks, rows = index.shape
    tiles = rows // LANES
    for block in range(blocks):
        listed = index[block : block + 1, :]
        live = lax.broadcasted_iota(jnp.int32, (1, rows), 1) < scalars[1 + block]
        high = jnp.where(live, listed // LANES, -1)
        low = listed % LANES
        high_hot = (lax.broadcasted_iota(jnp.int32, (tiles, rows), 0) == high).astype(f32).astype(bf16)
        low_hot = (lax.broadcasted_iota(jnp.int32, (LANES, rows), 0) == low).astype(f32).astype(bf16)
        chosen = contract_lanes(high_hot, low_hot)
        chosen = jnp.concatenate([chosen[t : t + 1, :] for t in range(tiles)], axis=1)
        offset = (place[...] - (scalars[0] + block)).astype(f32) / SPAN
        taper = 1.0 / (1.0 + offset * offset)
        factor_out[block : block + 1, :] = jnp.where(chosen > 0.5, weight[...] * taper, 0.0)


def gain_kernel(pred, factor, gain_out, pred_buf, sem):
    members, rows = pred.shape
    load = pltpu.make_async_copy(pred, pred_buf, sem)
    load.start()
    load.wait()
    values = from_middle(pred_buf[...].astype(f32))
    deviation = values - jnp.mean(values, axis=0, keepdims=True)
    eye = (
        lax.broadcasted_iota(jnp.int32, (members, members), 0)
        == lax.broadcasted_iota(jnp.int32, (members, members), 1)
    ).astype(f32)
    for block in range(factor.shape[0]):
        scaled = (factor[block : block + 1, :] * deviation * (1.0 / math.sqrt(members - 1.0))).astype(bf16)
        gram = contract_lanes(scaled, scaled)
        start = 2.0 / (2.0 + jnp.sqrt(jnp.sum(gram * gram)))
        residual = eye - start * (eye + gram)
        estimate = eye + residual
        residual_parts = split(residual)
        for step in range(1, NS_STEPS):
            residual = dot3(residual_parts, residual_parts)
            residual_parts = split(residual)
            estimate = estimate + dot3(split(estimate), residual_parts)
        high, low = split(estimate * (start * (1.0 / math.sqrt(members - 1.0))))
        gain_out[:, block * members : (block + 1) * members] = (contract_rows(scaled, high) + contract_rows(scaled, low)).astype(bf16)


def update_kernel(second, factor, pred, gain, updated, pred_buf, gain_buf, pred_sems, gain_sems):
    blocks, rows = factor.shape
    members = pred.shape[0]
    width = (second.shape[1] - rows) // blocks
    piece = rows // PIECES
    pred_loads, gain_loads = [], []
    for part in range(PIECES):
        span = pl.ds(part * piece, piece)
        pred_loads.append(pltpu.make_async_copy(pred.at[:, span], pred_buf.at[:, span], pred_sems.at[part]))
        gain_loads.append(pltpu.make_async_copy(gain.at[span, :], gain_buf.at[span, :], gain_sems.at[part]))
        pred_loads[part].start()
        gain_loads[part].start()
    weights_t = [None] * blocks
    for part in range(PIECES):
        span = slice(part * piece, (part + 1) * piece)
        pred_loads[part].wait()
        change = second[:, span].astype(f32) - from_middle(pred_buf[:, span].astype(f32))
        gain_loads[part].wait()
        for block in range(blocks):
            innovation = (factor[block : block + 1, span] * change).astype(bf16)
            product = dot(innovation, gain_buf[span, block * members : (block + 1) * members])
            weights_t[block] = product if part == 0 else weights_t[block] + product
    for block in range(blocks):
        span = slice(rows + block * width, rows + (block + 1) * width)
        cells = second[:, span].astype(f32)
        centred = (cells - jnp.mean(cells, axis=0, keepdims=True)).astype(bf16)
        total = from_last(cells + dot(weights_t[block].astype(bf16), centred))
        updated[:, block * width : (block + 1) * width] = total.astype(bf16)


def call(kernel, outs, flops, grant=None, scalars=0, stay=(), scratch=()):
    vmem = pl.BlockSpec(memory_space=pltpu.VMEM)
    smem = pl.BlockSpec(memory_space=pltpu.SMEM)
    hbm = pl.BlockSpec(memory_space=pltpu.HBM)

    def run(*args):
        specs = [smem] * scalars + [vmem] * (len(args) - scalars)
        for place in stay:
            specs[place] = hbm
        args = [
            pltpu.with_memory_space_constraint(arg, pltpu.HBM) if place in stay else arg
            for place, arg in enumerate(args)
        ]
        return pl.pallas_call(
            kernel,
            out_shape=outs,
            in_specs=specs,
            out_specs=vmem,
            scratch_shapes=list(scratch),
            cost_estimate=pl.CostEstimate(flops=flops, transcendentals=0, bytes_accessed=1 << 22),
            compiler_params=pltpu.CompilerParams(vmem_limit_bytes=grant),
            name=kernel.__name__,
        )(*args)

    return run


def per_device(state, predicted, perturbed, obs_weight, obs_position, row_count, row_index):
    def exchange(value, order=None):
        chunks = value.reshape(held, groups, -1)
        received = lax.all_to_all(
            chunks, "member", split_axis=1, concat_axis=0, tiled=True, axis_index_groups=order
        )
        return received.reshape(members, -1)

    groups = lax.axis_size("member")
    group_index = lax.axis_index("member")
    tile_index = lax.axis_index("domain")
    blocks = row_index.shape[1]
    held = state.shape[0]
    members = held * groups
    rows = predicted.shape[1] // groups
    cells = state.shape[1] // groups
    half = groups // 2
    middle_first = [[(half + spot) % groups for spot in range(groups)]]
    last_first = [list(range(groups))[::-1]]

    pred_pool = exchange(predicted)
    counts = lax.dynamic_index_in_dim(row_count, tile_index, 0, keepdims=False)
    first_block = (tile_index * groups + group_index) * blocks
    scalars = jnp.concatenate([first_block[None].astype(jnp.int32), counts])
    weight = lax.dynamic_slice_in_dim(obs_weight, group_index * rows, rows)[None]
    place = lax.dynamic_slice_in_dim(obs_position, group_index * rows, rows)[None]

    shaped = jax.ShapeDtypeStruct
    cube = 2 * blocks * members**3
    factor = call(factor_kernel, shaped((blocks, rows), f32), cube, 67043328, 1)(scalars, row_index[0], weight, place)
    paired = jnp.concatenate(
        [perturbed.reshape(held, groups, rows), state.reshape(held, groups, cells)], axis=2
    )
    factor, paired = lax.optimization_barrier((factor, jnp.flip(paired.reshape(held, 2, -1), axis=1)))
    second = exchange(paired, middle_first)
    gain = call(
        gain_kernel,
        shaped((rows, blocks * members), bf16),
        40 * cube,
        stay=(0,),
        scratch=(pltpu.VMEM((members, rows), bf16), pltpu.SemaphoreType.DMA),
    )(pred_pool, factor)
    updated = call(
        update_kernel,
        shaped((members, cells), bf16),
        5 * cube,
        grant=24 << 20,
        stay=(2, 3),
        scratch=(
            pltpu.VMEM((members, rows), bf16),
            pltpu.VMEM(gain.shape, bf16),
            pltpu.SemaphoreType.DMA((PIECES,)),
            pltpu.SemaphoreType.DMA((PIECES,)),
        ),
    )(second, factor, pred_pool, gain)
    returned = lax.all_to_all(
        updated, "member", split_axis=0, concat_axis=1, tiled=True, axis_index_groups=last_first
    )
    return jnp.flip(returned.reshape(held, groups, cells), axis=1).reshape(held, -1)


def solution(mesh):
    placed = (
        P("member", "domain"),
        P("member", "domain"),
        P("member", "domain"),
        P("domain"),
        P("domain"),
        P(None, "member"),
        P("domain", "member", None),
    )
    return jax.shard_map(
        per_device, mesh=mesh, in_specs=placed, out_specs=P("member", "domain"), check_vma=False
    )
```
